32 devices in a mesh: chain: 16 (over z, y, x), grp: 2 (over core).
Axes of the slice: x: 2, y: 2, z: 4, core: 2. Of those that a mesh axis runs over, the one named last changes fastest.
Arguments:
- codes: bfloat16 [2, 16384, 6144], P(None, ('chain', 'grp')), may hold values from -6 to 6
- exponents: int32 [2, 512, 6144], P(None, ('chain', 'grp')), may hold values from -2 to 2
- column_map: int32 [32], replicated, may hold values from 0 to 31, each once
- row_order: int32 [32], replicated, may hold values from 0 to 31, each once
Outputs:
- rollout: bfloat16 [2, 6144, 16384], P(None, ('chain', 'grp'))
- block_sums: float32 [2, 6144, 512], P(None, ('chain', 'grp'))
The draws below stay inside these ranges and needn't reach their ends.
All inputs are finite; a program needn't handle non-finite values.
Results may differ from the reference program's by a relative error of at most 0.001.
Values may be sent and summed in bfloat16 or wider, within the bound.
No kernel may reach another device: no remote copies, remote signals or barrier semaphores. Data moves between devices by JAX's collectives and lax.ppermute only.
A program may use at most 128 MiB of HBM per device.

```python
import jax
import jax.numpy as jnp

R = 16384
C = 6144
LAYERS = 2
N_CHAIN = 16
N_GRP = 2


def plant(result, key, low, largest):
    shape = result.shape
    place = [jax.random.randint(jax.random.fold_in(key, axis), (), 0, shape[axis]) for axis in range(len(shape))]
    result = result.at[tuple(place)].set(low)
    longest = shape.index(max(shape))
    place[longest] = (place[longest] + 1) % shape[longest]
    return result.at[tuple(place)].set(largest)


def block_levels(stream_key, extent, pieces, least, largest):
    def one(dim, parts):
        heights = jax.random.uniform(jax.random.fold_in(jax.random.fold_in(stream_key, 6), dim), (parts,), jnp.float32, least / len(pieces), largest / len(pieces))
        return jnp.repeat(jnp.exp(heights), extent[dim] // parts).reshape((-1,) + (1,) * (len(extent) - dim - 1))

    factor_of = one(*pieces[0])
    for cut in pieces[1:]:
        factor_of = factor_of * one(*cut)
    return factor_of


def gaussian(rng, shape, deviation, limit, shards=(), kind=jnp.bfloat16):
    result = jax.random.normal(rng, shape, jnp.float32) * deviation
    if len(shards) > 0:
        result = block_levels(rng, shape, shards, -0.22, 0.18) * result
    return jnp.clip(result, min=-limit, max=limit).astype(kind)


def setup_inputs(seed: int = 0) -> dict:
    arg_keys = jax.random.split(jax.random.key(seed), 5)
    return {
        "codes": gaussian(arg_keys[0], (LAYERS, R, C), 1.0, 6.0, ((1, 32),)),
        "exponents": plant(jax.random.randint(arg_keys[1], (LAYERS, R // 32, C), -2, 3), jax.random.fold_in(arg_keys[1], 1), -2, 2).astype(jnp.int32),
        "column_map": jax.random.permutation(arg_keys[2], N_CHAIN * N_GRP).astype(jnp.int32),
        "row_order": jax.random.permutation(arg_keys[3], N_CHAIN * N_GRP).astype(jnp.int32),
    }


def reference(codes, exponents, column_map, row_order):
    devices = N_CHAIN * N_GRP
    col_width = C // devices
    row_count = R // devices
    scaling = jnp.exp2(exponents.astype(jnp.float32))
    values = (codes.astype(jnp.float32) * jnp.repeat(scaling, 32, axis=1)).astype(jnp.bfloat16)
    col_index = (column_map[:, None] * col_width + jnp.arange(col_width, dtype=jnp.int32)[None, :]).reshape(-1)
    row_index = (row_order[:, None] * row_count + jnp.arange(row_count, dtype=jnp.int32)[None, :]).reshape(-1)
    picked = jnp.take(values, row_index.astype(jnp.int32), axis=1)
    picked = jnp.take(picked, col_index.astype(jnp.int32), axis=2)
    rollout = jnp.transpose(picked, (0, 2, 1))
    block_sums = rollout.astype(jnp.float32).reshape(LAYERS, C, R // 32, 32).sum(axis=-1)
    return rollout, block_sums
```

```python
import functools
import math

import jax
import jax.numpy as jnp
from jax import lax
from jax.experimental import pallas as pl
from jax.experimental.pallas import tpu as pltpu
from jax.sharding import PartitionSpec as P

AXES = ("chain", "grp")
BLOCK = 32
LANES = 128


def arrange(array, column_map, devices, col_width):
    layer_count, row_count, _ = array.shape
    order = (
        jnp.arange(col_width, dtype=jnp.int32)[:, None] + column_map[None, :] * col_width
    ).reshape(-1)
    picked = jnp.take(array, order, axis=2)
    return jnp.swapaxes(picked, 1, 2).reshape(layer_count, col_width, devices, row_count)


def plain(codes, exponents, column_map, row_order):
    chain_size = lax.axis_size("chain")
    grp_size = lax.axis_size("grp")
    devices = chain_size * grp_size
    layer_count, row_count, width_all = codes.shape
    col_width = width_all // devices
    scaling = jnp.exp2(exponents.astype(jnp.float32))
    values = (codes.astype(jnp.float32) * jnp.repeat(scaling, BLOCK, axis=1)).astype(jnp.bfloat16)
    outgoing = arrange(values, column_map, devices, col_width)
    shaped = outgoing.reshape(layer_count, col_width, chain_size, grp_size, row_count)
    arrived = lax.all_to_all(
        lax.all_to_all(shaped, "chain", split_axis=2, concat_axis=2, tiled=True),
        "grp",
        split_axis=3,
        concat_axis=3,
        tiled=True,
    )
    arrived = arrived.reshape(layer_count, col_width, devices, row_count)
    rollout = jnp.take(arrived, row_order, axis=2).reshape(layer_count, col_width, devices * row_count)
    block_sums = (
        rollout.astype(jnp.float32)
        .reshape(layer_count, col_width, devices * row_count // BLOCK, BLOCK)
        .sum(axis=-1)
    )
    return rollout, block_sums


def pack_kernel(where_ref, codes_ref, exponents_ref, out_ref, turned, *, col_width, group):
    member = pl.program_id(1)
    rows = codes_ref.shape[1]

    @pl.when(member == 0)
    def _():
        scaling = jnp.exp2(exponents_ref[0].astype(jnp.float32)).astype(jnp.bfloat16)
        for tile in range(col_width * group // LANES):
            lanes = slice(tile * LANES, (tile + 1) * LANES)
            parts = [
                codes_ref[0, b * BLOCK : (b + 1) * BLOCK, lanes] * scaling[b : b + 1, lanes]
                for b in range(rows // BLOCK)
            ]
            turned[lanes, :] = jnp.concatenate(parts, axis=0).T

    out_ref[0] = turned[pl.ds(pl.multiple_of(member * col_width, 16), col_width), :]


def pack(codes, exponents, where, layer, devices):
    _, rows, width_all = codes.shape
    col_width = width_all // devices
    group = math.lcm(col_width, LANES) // col_width
    wide = col_width * group
    return pl.pallas_call(
        functools.partial(pack_kernel, col_width=col_width, group=group),
        grid_spec=pltpu.PrefetchScalarGridSpec(
            num_scalar_prefetch=1,
            grid=(devices // group, group),
            in_specs=[
                pl.BlockSpec((1, rows, wide), lambda g, m, where: (layer, 0, g)),
                pl.BlockSpec((1, rows // BLOCK, wide), lambda g, m, where: (layer, 0, g)),
            ],
            out_specs=pl.BlockSpec(
                (1, col_width, rows), lambda g, m, where: (where[g * group + m], 0, 0)
            ),
            scratch_shapes=[pltpu.VMEM((wide, rows), jnp.bfloat16)],
        ),
        out_shape=jax.ShapeDtypeStruct((devices, col_width, rows), jnp.bfloat16),
        name=f"pack{layer}",
    )(where, codes, exponents)


def place_kernel(order_ref, *refs, take, rows):
    pieces, (rollout_ref, sums_ref) = refs[:take], refs[-2:]
    blocks = rows // BLOCK
    source = lax.broadcasted_iota(jnp.int32, (rows, take * blocks), 0) // BLOCK
    target = lax.broadcasted_iota(jnp.int32, (rows, take * blocks), 1)
    total = None
    for k, piece in enumerate(pieces):
        values = piece[0]
        rollout_ref[0, :, k * rows : (k + 1) * rows] = values
        mask = (source + k * blocks == target).astype(jnp.bfloat16)
        part = jnp.dot(values, mask, preferred_element_type=jnp.float32)
        total = part if total is None else total + part
    sums_ref[0] = total


def place(arrived, order, layer, layer_count, previous):
    devices, col_width, rows = arrived.shape
    take = LANES * BLOCK // rows
    piece = lambda k: pl.BlockSpec(
        (1, col_width, rows), lambda s, order: (order[s * take + k], 0, 0)
    )
    carried = [] if previous is None else list(previous)
    return pl.pallas_call(
        functools.partial(place_kernel, take=take, rows=rows),
        grid_spec=pltpu.PrefetchScalarGridSpec(
            num_scalar_prefetch=1,
            grid=(devices // take,),
            in_specs=[piece(k) for k in range(take)]
            + [pl.BlockSpec(memory_space=pl.ANY)] * len(carried),
            out_specs=[
                pl.BlockSpec((1, col_width, take * rows), lambda s, order: (layer, 0, s)),
                pl.BlockSpec((1, col_width, LANES), lambda s, order: (layer, 0, s)),
            ],
        ),
        out_shape=[
            jax.ShapeDtypeStruct((layer_count, col_width, devices * rows), jnp.bfloat16),
            jax.ShapeDtypeStruct((layer_count, col_width, devices * rows // BLOCK), jnp.float32),
        ],
        input_output_aliases={1 + take + i: i for i in range(len(carried))},
        name=f"place{layer}",
    )(order, *[arrived] * take, *carried)


def shards(codes, exponents, column_map, row_order):
    devices = lax.axis_size("chain") * lax.axis_size("grp")
    layer_count, rows, width_all = codes.shape
    col_width = width_all // devices
    whole_tiles = (
        rows % LANES == 0
        and LANES * BLOCK % rows == 0
        and devices % (LANES * BLOCK // rows) == 0
        and col_width % 16 == 0
        and devices % (math.lcm(col_width, LANES) // col_width) == 0
    )
    if not whole_tiles:
        return plain(codes, exponents, column_map, row_order)
    where = jnp.sum(
        jnp.where(
            column_map[None, :] == jnp.arange(devices, dtype=jnp.int32)[:, None],
            jnp.arange(devices, dtype=jnp.int32)[None, :],
            0,
        ),
        axis=1,
        dtype=jnp.int32,
    )
    arrived = [
        lax.all_to_all(
            pack(codes, exponents, where, layer, devices), AXES, split_axis=0, concat_axis=0, tiled=True
        )
        for layer in range(layer_count)
    ]
    done = None
    for layer in range(layer_count):
        done = place(arrived[layer], row_order, layer, layer_count, done)
    return tuple(done)


def solution(mesh):
    return jax.shard_map(
        shards,
        mesh=mesh,
        in_specs=(P(None, AXES, None), P(None, AXES, None), P(), P()),
        out_specs=(P(None, AXES, None), P(None, AXES, None)),
        check_vma=False,
    )
```

```python
import functools
import itertools
import math

import jax
import jax.numpy as jnp
import numpy as np
from jax import lax
from jax.experimental import pallas as pl
from jax.experimental.pallas import tpu as pltpu
from jax.sharding import PartitionSpec as P


AXES = ("chain", "grp")
BLOCK = 32
LANES = 128


def arrange(array, column_map, devices, col_width):
    layer_count, row_count, _ = array.shape
    order = (
        jnp.arange(col_width, dtype=jnp.int32)[:, None] + column_map[None, :] * col_width
    ).reshape(-1)
    picked = jnp.take(array, order, axis=2)
    return jnp.swapaxes(picked, 1, 2).reshape(layer_count, col_width, devices, row_count)


def plain(codes, exponents, column_map, row_order):
    chain_size = lax.axis_size("chain")
    grp_size = lax.axis_size("grp")
    devices = chain_size * grp_size
    layer_count, row_count, width_all = codes.shape
    col_width = width_all // devices
    scaling = jnp.exp2(exponents.astype(jnp.float32))
    values = (codes.astype(jnp.float32) * jnp.repeat(scaling, BLOCK, axis=1)).astype(jnp.bfloat16)
    outgoing = arrange(values, column_map, devices, col_width)
    shaped = outgoing.reshape(layer_count, col_width, chain_size, grp_size, row_count)
    arrived = lax.all_to_all(
        lax.all_to_all(shaped, "chain", split_axis=2, concat_axis=2, tiled=True),
        "grp",
        split_axis=3,
        concat_axis=3,
        tiled=True,
    )
    arrived = arrived.reshape(layer_count, col_width, devices, row_count)
    rollout = jnp.take(arrived, row_order, axis=2).reshape(layer_count, col_width, devices * row_count)
    block_sums = (
        rollout.astype(jnp.float32)
        .reshape(layer_count, col_width, devices * row_count // BLOCK, BLOCK)
        .sum(axis=-1)
    )
    return rollout, block_sums


def places_of(mesh):
    spots = np.array([(*d.coords, d.core_on_chip) for d in mesh.devices.flat])
    spots -= spots.min(axis=0)
    sizes = spots.max(axis=0) + 1
    axes = sorted(range(3), key=lambda a: -sizes[a]) + [3]
    return spots[:, axes], sizes[axes]


def routes(mesh):
    spots, sizes = places_of(mesh)
    number = {tuple(spot): i for i, spot in enumerate(spots.tolist())}
    side = [
        offset
        for offset in itertools.product(*(range(n) for n in sizes[1:]))
    ]
    side.sort(key=lambda offset: (-sum(offset[:-1]), -offset[0], offset[-1]))
    length = int(sizes[0])

    def step(shift, offset):
        targets = []
        for spot in spots.tolist():
            far = shift(spot) if callable(shift) else shift
            moved = [(a + b) % n for a, b, n in zip(spot, (far, *offset), sizes.tolist())]
            targets.append(number[tuple(moved)])
        return targets

    steps = []
    half = [step(length // 2, o) for o in side] if length % 2 == 0 else []
    near = [step(0, o) for o in side if any(o)]
    for pair in itertools.zip_longest(half, near):
        steps += [p for p in pair if p is not None]
    for shift in range(1, (length + 1) // 2):
        for offset in side:
            for turn in (0, 1):
                steps.append(
                    step(lambda spot: shift if (spot[-1] + turn) % 2 == 0 else length - shift, offset)
                )
    target = np.array(steps, np.int32)
    return target, np.argsort(target, axis=1).astype(np.int32)


def pack_kernel(column_ref, *refs, windows, col_width, step):
    codes, exponents = refs[:windows], refs[windows : 2 * windows]
    out_ref, turned = refs[2 * windows :]
    rows = codes[0].shape[1]
    for tile, (code, exponent) in enumerate(zip(codes, exponents)):
        scaling = jnp.exp2(exponent[0].astype(jnp.float32)).astype(jnp.bfloat16)
        parts = [
            code[0, b * BLOCK : (b + 1) * BLOCK, :] * scaling[b : b + 1, :]
            for b in range(rows // BLOCK)
        ]
        turned[tile * LANES : (tile + 1) * LANES, :] = jnp.concatenate(parts, axis=0).T
    offset = lax.rem(column_ref[step] * col_width, LANES)
    out_ref[0] = turned[pl.ds(pl.multiple_of(offset, 16), col_width), :]


def pack(codes, exponents, column, step, devices):
    layer_count, rows, width_all = codes.shape
    col_width = width_all // devices
    windows = -(-(LANES - math.gcd(col_width, LANES) + col_width) // LANES)
    last = width_all // LANES - 1

    def window(height, tile):
        return pl.BlockSpec(
            (1, height, LANES),
            lambda layer, column: (
                layer, 0, jnp.minimum(lax.div(column[step] * col_width, LANES) + tile, last)
            ),
        )

    return pl.pallas_call(
        functools.partial(pack_kernel, windows=windows, col_width=col_width, step=step),
        grid_spec=pltpu.PrefetchScalarGridSpec(
            num_scalar_prefetch=1,
            grid=(layer_count,),
            in_specs=[window(rows, tile) for tile in range(windows)]
            + [window(rows // BLOCK, tile) for tile in range(windows)],
            out_specs=pl.BlockSpec((1, col_width, rows), lambda layer, column: (layer, 0, 0)),
            scratch_shapes=[pltpu.VMEM((windows * LANES, rows), jnp.bfloat16)],
        ),
        out_shape=jax.ShapeDtypeStruct((layer_count, col_width, rows), jnp.bfloat16),
    )(column, *[codes] * windows, *[exponents] * windows)


def place_kernel(spot_ref, *refs, steps, first):
    count = len(steps)
    pieces = refs[:count]
    rollout, sums, held, total, came, left, moved = refs[-7:]
    layers, _, rows = held.shape[1:]
    per_tile = LANES * BLOCK // rows
    arrivals = [pltpu.make_async_copy(pieces[k], held.at[k], came.at[k]) for k in range(count)]
    for copy in arrivals:
        copy.start()
    if first:
        total[...] = jnp.zeros_like(total)
    else:
        so_far = pltpu.make_async_copy(refs[count + 1], total, moved.at[0])
        so_far.start()
        so_far.wait()
    block = lax.broadcasted_iota(jnp.int32, (rows, LANES), 0) // BLOCK
    lane = lax.broadcasted_iota(jnp.int32, (rows, LANES), 1)
    leavings = []
    for k, step in enumerate(steps):
        spot = spot_ref[step]
        arrivals[k].wait()
        leaving = pltpu.make_async_copy(
            held.at[k], rollout.at[:, :, pl.ds(pl.multiple_of(spot * rows, LANES), rows)], left.at[k]
        )
        leaving.start()
        leavings.append(leaving)
        mask = (block + lax.rem(spot, per_tile) * (rows // BLOCK) == lane).astype(jnp.bfloat16)
        tile = pl.ds(pl.multiple_of(lax.div(spot, per_tile) * LANES, LANES), LANES)
        for layer in range(layers):
            total[layer, :, tile] += jnp.dot(held[k, layer], mask, preferred_element_type=jnp.float32)
    last = pltpu.make_async_copy(total, sums, moved.at[1])
    last.start()
    for copy in leavings:
        copy.wait()
    last.wait()


def place(pieces, steps, spot, devices, previous):
    layer_count, col_width, rows = pieces[0].shape
    count = len(pieces)
    carried = [] if previous is None else list(previous)
    whole = jax.ShapeDtypeStruct((layer_count, col_width, devices * rows), jnp.bfloat16)
    sums = jax.ShapeDtypeStruct((layer_count, col_width, devices * rows // BLOCK), jnp.float32)
    anywhere = pl.BlockSpec(memory_space=pl.ANY)
    return pl.pallas_call(
        functools.partial(place_kernel, steps=steps, first=previous is None),
        grid_spec=pltpu.PrefetchScalarGridSpec(
            num_scalar_prefetch=1,
            grid=(1,),
            in_specs=[anywhere] * (count + len(carried)),
            out_specs=[anywhere, anywhere],
            scratch_shapes=[
                pltpu.VMEM((count, layer_count, col_width, rows), jnp.bfloat16),
                pltpu.VMEM(sums.shape, jnp.float32),
                pltpu.SemaphoreType.DMA((count,)),
                pltpu.SemaphoreType.DMA((count,)),
                pltpu.SemaphoreType.DMA((2,)),
            ],
        ),
        out_shape=[whole, sums],
        input_output_aliases={1 + count + i: i for i in range(len(carried))},
    )(spot, *pieces, *carried)


def lookup(table, index):
    hit = index[:, None] == jnp.arange(table.shape[0], dtype=jnp.int32)[None, :]
    return jnp.sum(jnp.where(hit, table[None, :], 0), axis=1, dtype=jnp.int32)


def groups_of(steps):
    sizes, left = [], steps
    for size in (2, 2, 4, 8):
        if left > 2 * size:
            sizes.append(size)
            left -= size
    while left > 0:
        sizes.append(min(left, 8))
        left -= sizes[-1]
    ends = np.cumsum(sizes[::-1])
    return [list(range(end - size, end)) for end, size in zip(ends, sizes[::-1])]


def shards(target, source, codes, exponents, column_map, row_order):
    devices = lax.axis_size("chain") * lax.axis_size("grp")
    if not fits(codes.shape, devices):
        return plain(codes, exponents, column_map, row_order)
    steps = len(target)
    me = lax.axis_index("chain") * lax.axis_size("grp") + lax.axis_index("grp")
    mine = (jnp.arange(devices, dtype=jnp.int32) == me)[None, :]
    itself = jnp.full((1,), me, jnp.int32)
    to = jnp.concatenate([jnp.sum(jnp.where(mine, target, 0), axis=1, dtype=jnp.int32), itself])
    came = jnp.concatenate([jnp.sum(jnp.where(mine, source, 0), axis=1, dtype=jnp.int32), itself])
    column = lookup(column_map, to)
    hit = came[:, None] == row_order[None, :]
    spot = jnp.sum(
        jnp.where(hit, jnp.arange(devices, dtype=jnp.int32)[None, :], 0), axis=1, dtype=jnp.int32
    )
    arrived = []
    for step in range(steps):
        piece = pack(codes, exponents, column, step, devices)
        arrived.append(lax.ppermute(piece, AXES, list(enumerate(target[step].tolist()))))
    arrived.append(pack(codes, exponents, column, steps, devices))
    done = None
    for number, group in enumerate(groups_of(steps)):
        if number == 0:
            group = [steps, *group]
        done = place([arrived[k] for k in group], group, spot, devices, done)
    return tuple(done)


def fits(shape, devices):
    _, rows, width_all = shape
    return (
        rows % LANES == 0
        and LANES * BLOCK % rows == 0
        and devices % (LANES * BLOCK // rows) == 0
        and width_all // devices % 16 == 0
        and width_all % LANES == 0
    )


def solution(mesh):
    target, source = routes(mesh)
    return jax.shard_map(
        functools.partial(shards, target, source),
        mesh=mesh,
        in_specs=(P(None, AXES, None), P(None, AXES, None), P(), P()),
        out_specs=(P(None, AXES, None), P(None, AXES, None)),
        check_vma=False,
    )
```

```python
import functools
import itertools
import math

import jax
import jax.numpy as jnp
import numpy as np
from jax import lax
from jax.experimental import pallas as pl
from jax.experimental.pallas import tpu as pltpu
from jax.sharding import PartitionSpec as P


AXES = ("chain", "grp")
BLOCK = 32
LANES = 128
VMEM_BYTES = 12 << 20
LATE = 1
LAST_GROUPS = (1, 2, 4, 8)


def arrange(array, column_map, devices, col_width):
    layer_count, row_count, _ = array.shape
    order = (
        jnp.arange(col_width, dtype=jnp.int32)[:, None] + column_map[None, :] * col_width
    ).reshape(-1)
    picked = jnp.take(array, order, axis=2)
    return jnp.swapaxes(picked, 1, 2).reshape(layer_count, col_width, devices, row_count)


def plain(codes, exponents, column_map, row_order):
    chain_size = lax.axis_size("chain")
    grp_size = lax.axis_size("grp")
    devices = chain_size * grp_size
    layer_count, row_count, width_all = codes.shape
    col_width = width_all // devices
    scaling = jnp.exp2(exponents.astype(jnp.float32))
    values = (codes.astype(jnp.float32) * jnp.repeat(scaling, BLOCK, axis=1)).astype(jnp.bfloat16)
    outgoing = arrange(values, column_map, devices, col_width)
    shaped = outgoing.reshape(layer_count, col_width, chain_size, grp_size, row_count)
    arrived = lax.all_to_all(
        lax.all_to_all(shaped, "chain", split_axis=2, concat_axis=2, tiled=True),
        "grp",
        split_axis=3,
        concat_axis=3,
        tiled=True,
    )
    arrived = arrived.reshape(layer_count, col_width, devices, row_count)
    rollout = jnp.take(arrived, row_order, axis=2).reshape(layer_count, col_width, devices * row_count)
    block_sums = (
        rollout.astype(jnp.float32)
        .reshape(layer_count, col_width, devices * row_count // BLOCK, BLOCK)
        .sum(axis=-1)
    )
    return rollout, block_sums


def places_of(mesh):
    spots = np.array([(*d.coords, d.core_on_chip) for d in mesh.devices.flat])
    spots -= spots.min(axis=0)
    sizes = spots.max(axis=0) + 1
    axes = sorted(range(3), key=lambda a: -sizes[a]) + [3]
    return spots[:, axes], sizes[axes]


def routes(mesh):
    spots, sizes = places_of(mesh)
    spots, sizes = spots.tolist(), sizes.tolist()
    number = {tuple(spot): i for i, spot in enumerate(spots)}
    length = sizes[0]
    side = list(itertools.product(*(range(n) for n in sizes[1:])))
    side.sort(key=lambda offset: (-sum(offset[:-1]), -offset[0], offset[-1]))

    def step(shift, offset):
        return [
            number[tuple((a + b) % n for a, b, n in zip(spot, (shift(spot), *offset), sizes))]
            for spot in spots
        ]

    def opposite(shift, turn):
        return lambda spot: shift if (spot[-1] + turn) % 2 == 0 else -shift

    mirror = lambda spot: length - 1 - 2 * spot[0]
    mirrored = length > 2 and all((length - 1 - 2 * z) % length in (1, length - 1) for z in range(length))
    half = [step(lambda spot: length // 2, o) for o in side[::-1]] if length % 2 == 0 else []
    near = [step(lambda spot: 0, o) for o in side if any(o)]
    steps, last = [], []
    if mirrored:
        steps.append(step(mirror, (0,) * len(side[0])))
        near.append(step(lambda spot: -mirror(spot), (0,) * len(side[0])))
    for pair in itertools.zip_longest(*((near, half) if mirrored else (half, near))):
        steps += [p for p in pair if p is not None]
    for shift in range(1, (length + 1) // 2):
        for offset in side:
            if mirrored and shift == 1 and not any(offset[:-1]):
                if any(offset):
                    last = [step(lambda spot: -mirror(spot), offset), step(mirror, offset)]
            else:
                steps += [step(opposite(shift, turn), offset) for turn in (0, 1)]
    steps += last
    target = np.array(steps, np.int32)
    return target, np.argsort(target, axis=1).astype(np.int32)


def pick(table, index):
    value = jnp.int32(int(table[0]))
    for i, entry in enumerate(table):
        value = jnp.where(index == i, jnp.int32(int(entry)), value)
    return value


def here():
    return lax.axis_index("chain") * lax.axis_size("grp") + lax.axis_index("grp")


OUTSIDE = pl.BlockSpec(memory_space=pltpu.HBM)
INSIDE = pl.BlockSpec(memory_space=pltpu.VMEM)
SCALARS = pl.BlockSpec(memory_space=pltpu.SMEM)


def keep(array, space):
    return pltpu.with_memory_space_constraint(array, space)


def pack_kernel(column_ref, codes, exponents, *refs, target, first, where):
    out_ref, raw, powers, turned, came = refs[:1] + refs[-4:]
    layers, rows, wide = raw.shape
    col_width = out_ref.shape[1]
    start = column_ref[pick(target, here())] * col_width
    tile = jnp.minimum(lax.div(start, LANES), (codes.shape[2] - wide) // LANES)
    lanes = pl.ds(pl.multiple_of(tile * LANES, LANES), wide)
    copies = []
    for layer in range(layers):
        copies.append(
            (
                pltpu.make_async_copy(codes.at[first + layer, :, lanes], raw.at[layer], came.at[layer, 0]),
                pltpu.make_async_copy(exponents.at[first + layer, :, lanes], powers.at[layer], came.at[layer, 1]),
            )
        )
        for copy in copies[-1]:
            copy.start()
    if where:
        for i in range(column_ref.shape[0]):
            refs[1][i] = column_ref[i]
    inner = pl.ds(pl.multiple_of(start - tile * LANES, 16), col_width)
    for layer in range(layers):
        for copy in copies[layer]:
            copy.wait()
        scaling = jnp.exp2(powers[layer].astype(jnp.float32)).astype(jnp.bfloat16)
        for part in range(wide // LANES):
            some = slice(part * LANES, (part + 1) * LANES)
            scaled = [
                raw[layer, b * BLOCK : (b + 1) * BLOCK, some] * scaling[b : b + 1, some]
                for b in range(rows // BLOCK)
            ]
            turned[layer, some, :] = jnp.concatenate(scaled, axis=0).T
        out_ref[layer] = turned[layer, inner, :]


def pack(codes, exponents, column_map, target, layers, where):
    _, rows, width_all = codes.shape
    col_width = width_all // len(target)
    count = len(layers)
    wide = -(-(LANES - math.gcd(col_width, LANES) + col_width) // LANES) * LANES
    return pl.pallas_call(
        functools.partial(pack_kernel, target=target, first=layers[0], where=where),
        in_specs=[SCALARS, OUTSIDE, OUTSIDE],
        out_specs=[INSIDE, SCALARS][: 1 + where],
        scratch_shapes=[
            pltpu.VMEM((count, rows, wide), jnp.bfloat16),
            pltpu.VMEM((count, rows // BLOCK, wide), jnp.int32),
            pltpu.VMEM((count, wide, rows), jnp.bfloat16),
            pltpu.SemaphoreType.DMA((count, 2)),
        ],
        out_shape=[
            pltpu.VMEM((count, col_width, rows), jnp.bfloat16),
            pltpu.SMEM(column_map.shape, jnp.int32),
        ][: 1 + where],
        compiler_params=pltpu.CompilerParams(vmem_limit_bytes=VMEM_BYTES),
    )(column_map, codes, exponents)


def spots_kernel(order_ref, spot_ref, *, sources):
    me = here()
    for step, source in enumerate(sources):
        wanted = pick(source, me)
        spot = jnp.int32(0)
        for k in range(order_ref.shape[0]):
            spot = jnp.where(order_ref[k] == wanted, k, spot)
        spot_ref[step] = spot


def place_kernel(spot_ref, *refs, parts, first, final):
    count = len(parts)
    pieces, (rollout, sums, total, left, moved) = refs[:count], refs[-5:]
    _, _, rows = pieces[0].shape
    per_tile = LANES * BLOCK // rows
    spots = [spot_ref[step] for step, _ in parts]
    copies = []

    def leave(source, target, semaphore):
        copies.append(pltpu.make_async_copy(source, target, semaphore))
        copies[-1].start()

    for k, (_, layers) in enumerate(parts):
        whole = pl.ds(pl.multiple_of(spots[k] * rows, LANES), rows)
        leave(pieces[k], rollout.at[layers[0] : layers[-1] + 1, :, whole], left.at[k])
    if first:
        total[...] = jnp.zeros_like(total)
    block = lax.broadcasted_iota(jnp.int32, (rows, LANES), 0) // BLOCK
    lane = lax.broadcasted_iota(jnp.int32, (rows, LANES), 1)
    tiles = [
        pl.ds(pl.multiple_of(lax.div(spot, per_tile) * LANES, LANES), LANES) for spot in spots
    ]
    for k, (_, layers) in enumerate(parts):
        mask = (block + lax.rem(spots[k], per_tile) * (rows // BLOCK) == lane).astype(jnp.bfloat16)
        for i, layer in enumerate(layers):
            total[layer, :, tiles[k]] += jnp.dot(pieces[k][i], mask, preferred_element_type=jnp.float32)
    if final == 1:
        leave(total, sums, moved.at[0])
    if final == 0:
        for k, (_, layers) in enumerate(parts):
            some = slice(layers[0], layers[-1] + 1)
            leave(total.at[some, :, tiles[k]], sums.at[some, :, tiles[k]], moved.at[k])
    for copy in copies:
        copy.wait()


def place(pieces, parts, spots, shape, previous, final):
    count = len(pieces)
    totals = (*shape[:-1], shape[-1] // BLOCK)
    carried = [] if previous is None else [previous[0], previous[1], keep(previous[2], pltpu.VMEM)]
    return pl.pallas_call(
        functools.partial(place_kernel, parts=parts, first=previous is None, final=final),
        in_specs=[SCALARS] + [INSIDE] * count + [OUTSIDE, OUTSIDE, INSIDE][: len(carried)],
        out_specs=[OUTSIDE, OUTSIDE, INSIDE],
        scratch_shapes=[pltpu.SemaphoreType.DMA((count,)), pltpu.SemaphoreType.DMA((count,))],
        out_shape=[
            jax.ShapeDtypeStruct(shape, jnp.bfloat16),
            jax.ShapeDtypeStruct(totals, jnp.float32),
            pltpu.VMEM(totals, jnp.float32),
        ],
        input_output_aliases={1 + count + i: i for i in range(len(carried))},
        compiler_params=pltpu.CompilerParams(vmem_limit_bytes=VMEM_BYTES),
    )(keep(spots, pltpu.SMEM), *[keep(piece, pltpu.VMEM) for piece in pieces], *carried)


def sends_of(steps, layer_count):
    every = tuple(range(layer_count))
    single = [(layer,) for layer in every]
    sends = [(0, layers) for layers in single] + [(step, every) for step in range(1, steps - LATE)]
    return sends + [(step, layers) for layers in single for step in range(steps - LATE, steps)]


def groups_of(sends):
    sizes, left = [], sends
    for size in LAST_GROUPS:
        if left > 2 * size:
            sizes.append(size)
            left -= size
    while left > 0:
        sizes.append(min(left, 8))
        left -= sizes[-1]
    ends = np.cumsum(sizes[::-1])
    return [list(range(end - size, end)) for end, size in zip(ends, sizes[::-1])]


def shards(target, source, codes, exponents, column_map, row_order):
    devices = lax.axis_size("chain") * lax.axis_size("grp")
    if not fits(codes.shape, devices):
        return plain(codes, exponents, column_map, row_order)
    codes, exponents, column_map, row_order = (
        keep(array, pltpu.HBM) for array in (codes, exponents, column_map, row_order)
    )
    layer_count, rows, width_all = codes.shape
    shape = (layer_count, width_all // devices, devices * rows)
    steps = len(target)
    itself = np.arange(devices)
    sends = sends_of(steps, layer_count)
    arrived = []
    for number, (step, layers) in enumerate(sends):
        piece, *columns = pack(codes, exponents, column_map, target[step], layers, number == 0)
        if columns:
            column_map = keep(columns[0], pltpu.SMEM)
        arrived.append(lax.ppermute(piece, AXES, list(enumerate(target[step].tolist()))))
    own = (steps, tuple(range(layer_count)))
    arrived += pack(codes, exponents, column_map, itself, own[1], False)
    parts = [*sends, own]
    spots = pl.pallas_call(
        functools.partial(spots_kernel, sources=[*source, itself]),
        in_specs=[SCALARS],
        out_specs=SCALARS,
        out_shape=pltpu.SMEM((steps + 1,), jnp.int32),
        compiler_params=pltpu.CompilerParams(vmem_limit_bytes=VMEM_BYTES),
        name="spots",
    )(row_order)
    done = None
    groups = groups_of(len(sends))
    groups[0].insert(0, len(sends))
    for number, group in enumerate(groups):
        done = place(
            [arrived[k] for k in group], [parts[k] for k in group], spots, shape, done,
            len(groups) - 1 - number,
        )
    return tuple(done[:2])


def fits(shape, devices):
    _, rows, width_all = shape
    return (
        rows % LANES == 0
        and LANES * BLOCK % rows == 0
        and devices % (LANES * BLOCK // rows) == 0
        and width_all // devices % 16 == 0
        and width_all % LANES == 0
    )


def solution(mesh):
    target, source = routes(mesh)

    inner = jax.shard_map(
        functools.partial(shards, target, source),
        mesh=mesh,
        in_specs=(P(None, AXES, None), P(None, AXES, None), P(), P()),
        out_specs=(P(None, AXES, None), P(None, AXES, None)),
        check_vma=False,
    )

    def step(codes, exponents, column_map, row_order):
        args = (codes, exponents, column_map, row_order)
        if not fits((codes.shape[0], codes.shape[1] // mesh.size, codes.shape[2]), mesh.size):
            return inner(*args)
        return inner(*args)

    return step
```
